32 devices in a mesh: dp: 4 (over y, z), tp: 8 (over x, core).
Axes of the slice: x: 4, y: 2, z: 2, core: 2. Of those that a mesh axis runs over, the one named last changes fastest.
The devices are a block of a 4x4x8 slice.
Arguments:
- query: bfloat16 [128, 64, 128], P('dp', 'tp'), parts along dimension 0
- k_cache: bfloat16 [128, 1024, 8, 128], P('dp', None, 'tp'), parts along dimension 0
- v_cache: bfloat16 [128, 1024, 8, 128], P('dp', None, 'tp'), parts along dimension 0
- k_new: bfloat16 [128, 8, 128], P('dp', 'tp'), parts along dimension 0
- v_new: bfloat16 [128, 8, 128], P('dp', 'tp'), parts along dimension 0
- lens: int32 [128], P('dp'), parts along dimension 0
Outputs:
- output 1: bfloat16 [128, 64, 128], P('dp', 'tp'), parts along dimension 0
- output 2: bfloat16 [128, 1024, 8, 128], P('dp', 'tp'), parts along dimension 0
- output 3: bfloat16 [128, 1024, 8, 128], P('dp', 'tp'), parts along dimension 0
There are 4 independent parts. The reference program is written for one: setup_inputs(seed, part) draws one part's arguments, and reference() takes and returns one part's arrays. A program takes and returns all parts, laid end to end along the dimension named above; each array names one.
All inputs are finite; a program needn't handle non-finite values.
Results may differ from the reference program's by a relative error of at most 0.00769032.
Values are sent between devices in bfloat16 or wider.
A program may use at most 768 MiB of HBM per device.

```python
import math
import jax
import jax.numpy as jnp
from jax import lax

BATCH = 32
SEQ_LEN = 1024
Q_HEADS = 64
KV_HEADS = 8
HEAD_DIM = 128


def setup_inputs(seed: int = 0, part: int = 0) -> dict:
    base_key = jax.random.fold_in(jax.random.key(seed), part)
    keys = jax.random.split(base_key, 6)
    group_size = Q_HEADS // KV_HEADS
    spread = math.sqrt(math.log(SEQ_LEN))
    align = 1.4 * math.sqrt(math.log(SEQ_LEN) / HEAD_DIM)
    cache_shape = (BATCH, SEQ_LEN, KV_HEADS, HEAD_DIM)
    k_cache = jax.random.normal(keys[0], cache_shape, jnp.float32)
    v_cache = jax.random.normal(keys[1], cache_shape, jnp.float32)
    k_new = jax.random.normal(keys[2], (BATCH, KV_HEADS, HEAD_DIM), jnp.float32)
    v_new = jax.random.normal(keys[3], (BATCH, KV_HEADS, HEAD_DIM), jnp.float32)
    noise = jax.random.normal(keys[4], (BATCH, KV_HEADS, group_size, HEAD_DIM), jnp.float32)
    mixed = math.sqrt(1.0 - align * align) * noise + align * k_new[:, :, None, :]
    query = (spread * mixed).reshape(BATCH, Q_HEADS, HEAD_DIM)
    len_keys = jax.random.split(keys[5])
    low_len = SEQ_LEN // 8
    lens = jax.random.randint(len_keys[0], (BATCH,), low_len, SEQ_LEN, jnp.int32)
    top_slot = jax.random.randint(len_keys[1], (), 0, BATCH, jnp.int32)
    lens = jnp.where(jnp.arange(BATCH) == top_slot, SEQ_LEN - 1, lens)
    return {"query": query.astype(jnp.bfloat16), "k_cache": k_cache.astype(jnp.bfloat16), "v_cache": v_cache.astype(jnp.bfloat16), "k_new": k_new.astype(jnp.bfloat16), "v_new": v_new.astype(jnp.bfloat16), "lens": lens}


def reference(query, k_cache, v_cache, k_new, v_new, lens):
    positions = jnp.arange(SEQ_LEN, dtype=jnp.int32)
    new_slot = (positions[None, :] == lens[:, None])[:, :, None, None]
    k_upd = jnp.where(new_slot, k_new[:, None], k_cache)
    v_upd = jnp.where(new_slot, v_new[:, None], v_cache)
    group_size = Q_HEADS // KV_HEADS
    inv_sqrt = HEAD_DIM ** -0.5

    def one_head(head_in):
        q_head, k_head, v_head, length = head_in
        scores = jnp.dot(q_head, k_head.T, preferred_element_type=jnp.float32) * inv_sqrt
        scores = jnp.where(positions[None, :] <= length, scores, -1e30)
        probs = jax.nn.softmax(scores, axis=-1)
        return jnp.dot(probs.astype(jnp.bfloat16), v_head, preferred_element_type=jnp.float32)

    q_flat = query.reshape(BATCH * KV_HEADS, group_size, HEAD_DIM)
    k_flat = jnp.swapaxes(k_upd, 1, 2).reshape(BATCH * KV_HEADS, SEQ_LEN, HEAD_DIM)
    v_flat = jnp.swapaxes(v_upd, 1, 2).reshape(BATCH * KV_HEADS, SEQ_LEN, HEAD_DIM)
    len_flat = jnp.repeat(lens, KV_HEADS)
    head_out = lax.map(one_head, (q_flat, k_flat, v_flat, len_flat))
    attn_out = head_out.reshape(BATCH, Q_HEADS, HEAD_DIM).astype(jnp.bfloat16)
    return attn_out, k_upd, v_upd
```

```python
import functools
import jax
import jax.numpy as jnp
from jax import lax
from jax.experimental import pallas as pl
from jax.experimental.pallas import tpu as pltpu
from jax.sharding import PartitionSpec as P

MASK_VALUE = -1e30
MESH = pl.DeviceIdType.MESH
REQS = 2


def exchange_kernel(n, lens_ref, q_ref, kn_ref, vn_ref, k_hbm, v_hbm,
                    out_ref, k_out, v_out,
                    recv, new_recv, new_all, new_own, k_buf, v_buf,
                    send_sem, recv_sem, new_send_sem, new_recv_sem, kv_sem):
    batch, seq_len, head_dim = k_hbm.shape
    seq_local = seq_len // n
    chunks = batch // REQS
    me = lax.axis_index("tp")
    group = lax.axis_index("dp")
    caches = (k_hbm, v_hbm)
    outs = (k_out, v_out)

    def peer(j):
        return lax.rem(me + j, n)

    barrier = pltpu.get_barrier_semaphore()
    for j in range(1, n):
        pl.semaphore_signal(barrier, inc=1, device_id=(group, peer(j)), device_id_type=MESH)
    pl.semaphore_wait(barrier, n - 1)

    def unit_copy(c, kv, j):
        dst_dev = peer(j)
        src = caches[kv].at[pl.ds(c * REQS, REQS), pl.ds(pl.multiple_of(dst_dev * seq_local, seq_local), seq_local)]
        dst = recv.at[c, kv, me]
        if j == 0:
            return pltpu.make_async_copy(src, dst, recv_sem.at[c, kv])
        return pltpu.make_async_remote_copy(src, dst, send_sem.at[c, kv], recv_sem.at[c, kv],
                                            device_id=(group, dst_dev), device_id_type=MESH)

    def new_copy(kv, j):
        src = (kn_ref, vn_ref)[kv]
        return pltpu.make_async_remote_copy(src, new_recv.at[kv, me], new_send_sem, new_recv_sem,
                                            device_id=(group, peer(j)), device_id_type=MESH)

    for kv in range(2):
        for j in range(1, n):
            new_copy(kv, j).start()

    def start_unit(c, carry):
        for kv in range(2):
            for j in (4, 3, 5, 2, 6, 1, 7, 0):
                unit_copy(c, kv, j).start()
        return carry

    lax.fori_loop(0, chunks, start_unit, 0)

    for kv in range(2):
        new_own[kv] = (kn_ref, vn_ref)[kv][...].astype(jnp.float32)

    def load(b, slot):
        return (pltpu.make_async_copy(k_hbm.at[b], k_buf.at[slot], kv_sem.at[slot, 0]),
                pltpu.make_async_copy(v_hbm.at[b], v_buf.at[slot], kv_sem.at[slot, 1]))

    for cp in load(0, 0):
        cp.start()
    scale = head_dim ** -0.5
    pos = lax.broadcasted_iota(jnp.int32, (1, seq_len), 1)

    def attend(b, carry):
        slot = lax.rem(b, 2)

        @pl.when(b + 1 < batch)
        def _():
            for cp in load(b + 1, 1 - slot):
                cp.start()

        for cp in load(b, slot):
            cp.wait()
        length = lens_ref[b]
        q = q_ref[b]
        qf = q.astype(jnp.float32)
        s = lax.dot_general(q, k_buf[slot], (((1,), (1,)), ((), ())), preferred_element_type=jnp.float32) * scale
        s_new = jnp.sum(qf * new_own[0, pl.ds(b, 1), :], axis=1, keepdims=True) * scale
        s = jnp.where(pos < length, s, MASK_VALUE)
        m = jnp.maximum(jnp.max(s, axis=1, keepdims=True), s_new)
        e = jnp.where(pos < length, jnp.exp(s - m), 0.0)
        e_new = jnp.exp(s_new - m)
        denom = jnp.sum(e, axis=1, keepdims=True) + e_new
        p = (e / denom).astype(jnp.bfloat16)
        p_new = (e_new / denom).astype(jnp.bfloat16).astype(jnp.float32)
        o = lax.dot_general(p, v_buf[slot], (((1,), (0,)), ((), ())), preferred_element_type=jnp.float32)
        o = o + p_new * new_own[1, pl.ds(b, 1), :]
        out_ref[b] = o.astype(jnp.bfloat16)
        return carry

    lax.fori_loop(0, batch, attend, 0)

    moved = new_recv.at[:, pl.ds(0, n - 1)]
    pltpu.make_async_copy(moved, moved, new_send_sem).wait()
    pltpu.make_async_copy(moved, moved, new_recv_sem).wait()
    for kv in range(2):
        new_recv[kv, me] = (kn_ref, vn_ref)[kv][...]
        new_all[kv] = jnp.swapaxes(new_recv[kv].astype(jnp.float32), 0, 1)

    tok = lax.broadcasted_iota(jnp.int32, (seq_local, n, head_dim), 0)

    def finish(c, carry):
        for kv in range(2):
            pltpu.make_async_copy(recv.at[c, kv], recv.at[c, kv], recv_sem.at[c, kv]).wait()
            for r in range(REQS):
                b = c * REQS + r
                at = lens_ref[b] - me * seq_local
                x = jnp.swapaxes(recv[c, kv, :, r].astype(jnp.float32), 0, 1)
                x = jnp.where(tok == at, new_all[kv, b][None], x)
                outs[kv][b] = x.astype(jnp.bfloat16)
        return carry

    lax.fori_loop(0, chunks, finish, 0)

    def drain(c, carry):
        for kv in range(2):
            sent = recv.at[c, kv, pl.ds(0, n - 1)]
            pltpu.make_async_copy(sent, sent, send_sem.at[c, kv]).wait()
        return carry

    lax.fori_loop(0, chunks, drain, 0)


def solution(mesh):
    n = mesh.shape["tp"]

    def local_step(query, k_cache, v_cache, k_new, v_new, lens):
        batch, seq_len, kv_heads, head_dim = k_cache.shape
        group = query.shape[1]
        chunks = batch // REQS
        seq_local = seq_len // n
        vmem = pl.BlockSpec(memory_space=pltpu.VMEM)
        anym = pl.BlockSpec(memory_space=pl.ANY)
        cache_out = jax.ShapeDtypeStruct((batch, seq_local, n * kv_heads, head_dim), k_cache.dtype)
        return pl.pallas_call(
            functools.partial(exchange_kernel, n),
            out_shape=(jax.ShapeDtypeStruct(query.shape, query.dtype), cache_out, cache_out),
            in_specs=[pl.BlockSpec(memory_space=pltpu.SMEM), vmem, vmem, vmem, anym, anym],
            out_specs=(vmem, vmem, vmem),
            scratch_shapes=[
                pltpu.VMEM((chunks, 2, n, REQS, seq_local, head_dim), jnp.bfloat16),
                pltpu.VMEM((2, n, batch, head_dim), jnp.bfloat16),
                pltpu.VMEM((2, batch, n, head_dim), jnp.float32),
                pltpu.VMEM((2, batch, head_dim), jnp.float32),
                pltpu.VMEM((2, seq_len, head_dim), jnp.bfloat16),
                pltpu.VMEM((2, seq_len, head_dim), jnp.bfloat16),
                pltpu.SemaphoreType.DMA((chunks, 2)),
                pltpu.SemaphoreType.DMA((chunks, 2)),
                pltpu.SemaphoreType.DMA,
                pltpu.SemaphoreType.DMA,
                pltpu.SemaphoreType.DMA((2, 2)),
            ],
            compiler_params=pltpu.CompilerParams(
                collective_id=0, has_side_effects=True, vmem_limit_bytes=62 * 1024 * 1024
            ),
            name="exchange",
        )(lens, query, k_new.reshape(batch, head_dim), v_new.reshape(batch, head_dim),
          k_cache.reshape(batch, seq_len, head_dim), v_cache.reshape(batch, seq_len, head_dim))

    head_spec = P("dp", "tp")
    entry_spec = P("dp", None, "tp")
    return jax.shard_map(local_step, mesh=mesh, in_specs=(head_spec, entry_spec, entry_spec, head_spec, head_spec, P("dp")), out_specs=(head_spec, P("dp", "tp"), P("dp", "tp")), check_vma=False)
```

```python
import functools
import jax
import jax.numpy as jnp
from jax import lax
from jax.experimental import pallas as pl
from jax.experimental.pallas import tpu as pltpu
from jax.sharding import PartitionSpec as P

MASK_VALUE = -1e30
MESH = pl.DeviceIdType.MESH
CHUNKS = (1, 1, 2, 4, 4, 4, 4, 4, 4, 2, 1, 1)
STORES = 4
LOADS = (1, 7, 8, 16)
ARRIVALS = (8, 8, 8, 4, 2, 1, 1)
HOPS = (4, 5, 3, 2, 6, 7, 1)


def spans(total, sizes):
    out, start = [], 0
    while start < total:
        size = min(sizes[min(len(out), len(sizes) - 1)], total - start)
        out.append(pl.ds(start, size))
        start += size
    return out


def span_of(total, sizes, b):
    return sum(b >= s.start for s in spans(total, sizes)[1:])


def exchange_kernel(n, lens_hbm, q_hbm, kn_hbm, vn_hbm, k_hbm, v_hbm,
                    out_ref, k_out, v_out,
                    lens_ref, q_ref, new_in, new_f32, kv, recv,
                    send_sem, recv_sem, load_sem, in_sem):
    batch, seq_len, head_dim = k_hbm.shape
    seq_local = seq_len // n
    me = lax.axis_index("tp")
    group = lax.axis_index("dp")
    outs = (k_out, v_out)

    barrier = pltpu.get_barrier_semaphore()
    for j in HOPS:
        pl.semaphore_signal(barrier, inc=1, device_id=(group, lax.rem(me + j, n)), device_id_type=MESH)

    def whole(ref, sem):
        return pltpu.make_async_copy(ref, ref, sem)

    small = (pltpu.make_async_copy(lens_hbm, lens_ref, in_sem.at[0]),
             pltpu.make_async_copy(kn_hbm, new_in.at[0], in_sem.at[1]),
             pltpu.make_async_copy(vn_hbm, new_in.at[1], in_sem.at[1]))
    query = pltpu.make_async_copy(q_hbm, q_ref, in_sem.at[2])
    load_spans = spans(batch, LOADS)

    def start_load(g):
        reqs = load_spans[g]
        pltpu.make_async_copy(k_hbm.at[reqs], kv.at[reqs, 0], load_sem.at[g]).start()
        pltpu.make_async_copy(v_hbm.at[reqs], kv.at[reqs, 1], load_sem.at[g]).start()

    for cp in small:
        cp.start()
    start_load(0)
    small[0].wait()
    whole(new_in, in_sem.at[1]).wait()
    new_f32[...] = new_in[...].astype(jnp.float32)

    row = lax.broadcasted_iota(jnp.int32, (seq_len, head_dim), 0)

    def insert_one(b, carry):
        at = lens_ref[b]
        for i in range(2):
            new = new_f32[i, pl.ds(b, 1), :].astype(kv.dtype)
            kv[b, i] = jnp.where(row == at, new, kv[b, i])
            recv[b, i, me] = kv[b, i, pl.ds(pl.multiple_of(me * seq_local, seq_local), seq_local)]
        return carry

    chunk_spans = spans(batch, CHUNKS)

    def insert(c):
        if c < len(chunk_spans):
            reqs = chunk_spans[c]
            for g, load in enumerate(load_spans):
                if load.start == reqs.start:
                    whole(kv.at[load], load_sem.at[g]).wait()
            lax.fori_loop(reqs.start, reqs.start + reqs.size, insert_one, 0)

    def send(c):
        reqs = chunk_spans[c]
        for j in HOPS:
            peer = lax.rem(me + j, n)
            pltpu.make_async_remote_copy(
                kv.at[reqs, :, pl.ds(pl.multiple_of(peer * seq_local, seq_local), seq_local)],
                recv.at[reqs, :, me], send_sem, recv_sem.at[span_of(batch, ARRIVALS, reqs.start)],
                device_id=(group, peer), device_id_type=MESH).start()

    insert(0)
    for g in range(1, len(load_spans)):
        start_load(g)
    query.start()
    pl.semaphore_wait(barrier, n - 1)
    send(0)
    insert(1)
    for c in range(1, len(chunk_spans)):
        insert(c + 1)
        send(c)
    query.wait()

    scale = head_dim ** -0.5
    pos = lax.broadcasted_iota(jnp.int32, (1, seq_len), 1)

    def attend(b, carry):
        s = lax.dot_general(q_ref[b], kv[b, 0], (((1,), (1,)), ((), ())), preferred_element_type=jnp.float32) * scale
        valid = pos <= lens_ref[b]
        s = jnp.where(valid, s, MASK_VALUE)
        e = jnp.exp(s - jnp.max(s, axis=1, keepdims=True))
        p = (e / jnp.sum(e, axis=1, keepdims=True)).astype(kv.dtype)
        o = lax.dot_general(p, kv[b, 1], (((1,), (0,)), ((), ())), preferred_element_type=jnp.float32)
        out_ref[b] = o.astype(out_ref.dtype)
        return carry

    lax.fori_loop(0, batch, attend, 0)

    def finish(b, carry):
        for i in range(2):
            x = jnp.swapaxes(recv[b, i].astype(jnp.float32), 0, 1)
            outs[i][b] = x.astype(kv.dtype)
        return carry

    for g, reqs in enumerate(spans(batch, ARRIVALS)):
        whole(recv.at[reqs, :, pl.ds(0, n - 1)], recv_sem.at[g]).wait()
        lax.fori_loop(reqs.start, reqs.start + reqs.size, finish, 0)

    whole(recv.at[:, :, pl.ds(0, n - 1)], send_sem).wait()


def store_kernel(out_in, k_in, v_in, out_hbm, k_hbm, v_hbm, sem):
    step = k_in.shape[0] // STORES
    pltpu.make_async_copy(out_in, out_hbm, sem.at[2]).start()
    for p in range(STORES):
        part = pl.ds(p * step, step)
        pltpu.make_async_copy(k_in.at[part], k_hbm.at[part], sem.at[0]).start()
        pltpu.make_async_copy(v_in.at[part], v_hbm.at[part], sem.at[1]).start()
    for i, ref in enumerate((k_in, v_in, out_in)):
        pltpu.make_async_copy(ref, ref, sem.at[i]).wait()


def solution(mesh):
    n = mesh.shape["tp"]

    def local_step(query, k_cache, v_cache, k_new, v_new, lens):
        batch, seq_len, kv_heads, head_dim = k_cache.shape
        seq_local = seq_len // n
        dtype = k_cache.dtype
        cache_out = pltpu.VMEM((batch, seq_local, n * kv_heads, head_dim), dtype)
        hbm = pl.BlockSpec(memory_space=pltpu.HBM)
        vmem = pl.BlockSpec(memory_space=pltpu.VMEM)
        held = pl.pallas_call(
            functools.partial(exchange_kernel, n),
            out_shape=(pltpu.VMEM(query.shape, query.dtype), cache_out, cache_out),
            in_specs=[hbm] * 6,
            out_specs=(vmem,) * 3,
            scratch_shapes=[
                pltpu.SMEM((batch,), jnp.int32),
                pltpu.VMEM(query.shape, query.dtype),
                pltpu.VMEM((2, batch, head_dim), dtype),
                pltpu.VMEM((2, batch, head_dim), jnp.float32),
                pltpu.VMEM((batch, 2, seq_len, head_dim), dtype),
                pltpu.VMEM((batch, 2, n, seq_local, head_dim), dtype),
                pltpu.SemaphoreType.DMA,
                pltpu.SemaphoreType.DMA((len(spans(batch, ARRIVALS)),)),
                pltpu.SemaphoreType.DMA((len(spans(batch, LOADS)),)),
                pltpu.SemaphoreType.DMA((3,)),
            ],
            compiler_params=pltpu.CompilerParams(
                collective_id=0, has_side_effects=True, vmem_limit_bytes=40 * 1024 * 1024
            ),
            name="exchange",
        )(lens, query, k_new.reshape(batch, head_dim), v_new.reshape(batch, head_dim),
          k_cache.reshape(batch, seq_len, head_dim), v_cache.reshape(batch, seq_len, head_dim))
        held = [pltpu.with_memory_space_constraint(h, pltpu.VMEM) for h in held]
        return pl.pallas_call(
            store_kernel,
            out_shape=tuple(jax.ShapeDtypeStruct(h.shape, h.dtype) for h in held),
            in_specs=[vmem] * 3,
            out_specs=(hbm,) * 3,
            scratch_shapes=[pltpu.SemaphoreType.DMA((3,))],
            compiler_params=pltpu.CompilerParams(vmem_limit_bytes=1024 * 1024),
            name="store",
        )(*held)

    head_spec = P("dp", "tp")
    entry_spec = P("dp", None, "tp")
    return jax.shard_map(local_step, mesh=mesh, in_specs=(head_spec, entry_spec, entry_spec, head_spec, head_spec, P("dp")), out_specs=(head_spec, P("dp", "tp"), P("dp", "tp")), check_vma=False)
```

```python
import functools
import jax
import jax.numpy as jnp
from jax import lax
from jax.experimental import pallas as pl
from jax.experimental.pallas import tpu as pltpu
from jax.sharding import PartitionSpec as P

MASK_VALUE = -1e30
VMEM_BYTES = 67043328
LESS_BYTES = VMEM_BYTES - 1536 * 1024
TILE = 16
PIECES = (4, 4, 10, 10, 3, 1)
EARLY = 2
HOPS = (4, 5, 3, 6, 2, 7, 1)


def whole(ref, sem):
    return pltpu.make_async_copy(ref, ref, sem)


def pack_kernel(n, reqs, hops, after, lens_hbm, kn_hbm, vn_hbm, k_hbm, v_hbm, *refs):
    blocks = refs[after:after + len(hops)]
    lens_ref, new_in, new_f32, kv, in_sem, load_sem, out_sem = refs[after + len(hops):]
    seq_len, head_dim = k_hbm.shape[1:]
    seq_local = seq_len // n
    me = lax.axis_index("tp")
    small = (pltpu.make_async_copy(lens_hbm, lens_ref, in_sem.at[0]),
             pltpu.make_async_copy(kn_hbm, new_in.at[0], in_sem.at[1]),
             pltpu.make_async_copy(vn_hbm, new_in.at[1], in_sem.at[1]))
    for cp in small:
        cp.start()
    starts = [lax.rem(me + j, n) * seq_local for j in hops]
    for h, first in enumerate(starts):
        rows = pl.ds(pl.multiple_of(first, seq_local), seq_local)
        pltpu.make_async_copy(k_hbm.at[reqs, rows], kv.at[h, :, 0], load_sem.at[h]).start()
        pltpu.make_async_copy(v_hbm.at[reqs, rows], kv.at[h, :, 1], load_sem.at[h]).start()
    small[0].wait()
    whole(new_in, in_sem.at[1]).wait()
    new_f32[...] = new_in[...].astype(jnp.float32)
    row = lax.broadcasted_iota(jnp.int32, (TILE, head_dim), 0)
    for h, first in enumerate(starts):
        whole(kv.at[h], load_sem.at[h]).wait()

        def insert(r, carry):
            at = lens_ref[reqs.start + r] - first
            tile = pl.ds(pl.multiple_of(jnp.clip(at, 0, seq_local - 1) // TILE * TILE, TILE), TILE)
            for i in range(2):
                new = new_f32[i, pl.ds(reqs.start + r, 1), :]
                old = kv[h, r, i, tile].astype(jnp.float32)
                kv[h, r, i, tile] = jnp.where(row == at - tile.start, new, old).astype(kv.dtype)
            return carry

        lax.fori_loop(0, reqs.size, insert, 0)
        pltpu.make_async_copy(kv.at[h], blocks[h], out_sem.at[h]).start()
    for h in range(len(hops)):
        whole(kv.at[h], out_sem.at[h]).wait()


def unpack_kernel(n, reqs, *refs):
    blocks = refs[:n]
    k_out, v_out, raw, held, in_sem, out_sem = refs[-6:]
    me = lax.axis_index("tp")
    copies = []
    for j in (*HOPS, 0):
        head = lax.rem(me + n - j, n)
        copies.append(pltpu.make_async_copy(blocks[j], raw.at[:, :, head], in_sem.at[j]))
        copies[-1].start()
    for cp in copies:
        cp.wait()

    def finish(r, carry):
        for i, out in enumerate((k_out, v_out)):
            x = jnp.swapaxes(raw[r, i].astype(jnp.float32), 0, 1)
            held[i, r] = x.astype(held.dtype)
            pltpu.make_async_copy(held.at[i, r], out.at[reqs.start + r], out_sem.at[i]).start()
        return carry

    lax.fori_loop(0, reqs.size, finish, 0)
    for i in range(2):
        whole(held.at[i], out_sem.at[i]).wait()


def attend_kernel(lens_hbm, q_hbm, kn_hbm, vn_hbm, k_hbm, v_hbm, after_hbm, out_ref,
                  lens_ref, q_ref, new_in, new_f32, kv, in_sem, kv_sem):
    batch, seq_len, head_dim = k_hbm.shape
    small = (pltpu.make_async_copy(lens_hbm, lens_ref, in_sem.at[0]),
             pltpu.make_async_copy(q_hbm, q_ref, in_sem.at[1]),
             pltpu.make_async_copy(kn_hbm, new_in.at[0], in_sem.at[2]),
             pltpu.make_async_copy(vn_hbm, new_in.at[1], in_sem.at[3]))
    for cp in small:
        cp.start()

    def load(b, slot):
        pltpu.make_async_copy(k_hbm.at[b], kv.at[slot, 0], kv_sem.at[slot]).start()
        pltpu.make_async_copy(v_hbm.at[b], kv.at[slot, 1], kv_sem.at[slot]).start()

    load(0, 0)
    for cp in small:
        cp.wait()
    new_f32[...] = new_in[...].astype(jnp.float32)
    scale = head_dim ** -0.5
    pos = lax.broadcasted_iota(jnp.int32, (1, seq_len), 1)

    def attend(b, carry):
        slot = lax.rem(b, 2)

        @pl.when(b + 1 < batch)
        def _():
            load(b + 1, 1 - slot)

        whole(kv.at[slot], kv_sem.at[slot]).wait()
        length = lens_ref[b]
        q = q_ref[b]
        s = lax.dot_general(q, kv[slot, 0], (((1,), (1,)), ((), ())), preferred_element_type=jnp.float32) * scale
        s_new = jnp.sum(q.astype(jnp.float32) * new_f32[0, pl.ds(b, 1), :], axis=1, keepdims=True) * scale
        s = jnp.where(pos < length, s, MASK_VALUE)
        m = jnp.maximum(jnp.max(s, axis=1, keepdims=True), s_new)
        e = jnp.where(pos < length, jnp.exp(s - m), 0.0)
        e_new = jnp.exp(s_new - m)
        denom = jnp.sum(e, axis=1, keepdims=True) + e_new
        p = (e / denom).astype(kv.dtype)
        p_new = (e_new / denom).astype(kv.dtype).astype(jnp.float32)
        o = lax.dot_general(p, kv[slot, 1], (((1,), (0,)), ((), ())), preferred_element_type=jnp.float32)
        out_ref[b] = (o + p_new * new_f32[1, pl.ds(b, 1), :]).astype(out_ref.dtype)
        return carry

    lax.fori_loop(0, batch, attend, 0)


def spans(total, sizes):
    out, start = [], 0
    while start < total:
        size = min(sizes[min(len(out), len(sizes) - 1)], total - start)
        out.append(pl.ds(start, size))
        start += size
    return out


def packs(p):
    return (HOPS[:EARLY], (*HOPS[EARLY:], 0)) if p == 0 else ((*HOPS, 0),)


def cost(flops, moved):
    return pl.CostEstimate(flops=flops, bytes_accessed=moved, transcendentals=0)


def solution(mesh):
    n = mesh.shape["tp"]

    def layer(query, k_cache, v_cache, k_new, v_new, lens):
        batch, seq_len, kv_heads, head_dim = k_cache.shape
        seq_local = seq_len // n
        dtype = k_cache.dtype
        hbm = pl.BlockSpec(memory_space=pltpu.HBM)
        keys, values = (x.reshape(batch, seq_len, head_dim) for x in (k_cache, v_cache))
        new_k, new_v = (x.reshape(batch, head_dim) for x in (k_new, v_new))
        row_bytes = 2 * 2 * seq_len * head_dim

        def pack(reqs, hops, after):
            block = jax.ShapeDtypeStruct((reqs.size, 2, seq_local, head_dim), dtype)
            return pl.pallas_call(
                functools.partial(pack_kernel, n, reqs, hops, len(after)),
                out_shape=(block,) * len(hops),
                in_specs=[hbm] * (5 + len(after)),
                out_specs=(hbm,) * len(hops),
                scratch_shapes=[
                    pltpu.SMEM((batch,), jnp.int32),
                    pltpu.VMEM((2, batch, head_dim), dtype),
                    pltpu.VMEM((2, batch, head_dim), jnp.float32),
                    pltpu.VMEM((len(hops), *block.shape), dtype),
                    pltpu.SemaphoreType.DMA((2,)),
                    pltpu.SemaphoreType.DMA((len(hops),)),
                    pltpu.SemaphoreType.DMA((len(hops),)),
                ],
                compiler_params=pltpu.CompilerParams(vmem_limit_bytes=LESS_BYTES if after else VMEM_BYTES),
                cost_estimate=cost(0, 2 * reqs.size * row_bytes * len(hops) // n),
            )(lens, new_k, new_v, keys, values, *after)

        def unpack(reqs, blocks, outs):
            cache = jax.ShapeDtypeStruct((batch, seq_local, n * kv_heads, head_dim), dtype)
            return pl.pallas_call(
                functools.partial(unpack_kernel, n, reqs),
                out_shape=(cache, cache),
                in_specs=[hbm] * (n + len(outs)),
                out_specs=(hbm, hbm),
                scratch_shapes=[
                    pltpu.VMEM((reqs.size, 2, n, seq_local, head_dim), dtype),
                    pltpu.VMEM((2, reqs.size, seq_local, n * kv_heads, head_dim), dtype),
                    pltpu.SemaphoreType.DMA((n,)),
                    pltpu.SemaphoreType.DMA((2,)),
                ],
                input_output_aliases={n + i: i for i in range(len(outs))},
                compiler_params=pltpu.CompilerParams(vmem_limit_bytes=LESS_BYTES),
                cost_estimate=cost(0, 2 * reqs.size * row_bytes),
            )(*blocks, *outs)

        pieces = spans(batch, PIECES)
        arrived = []
        after = ()
        for p, reqs in enumerate(pieces):
            blocks = {}
            for hops in packs(p):
                packed = pack(reqs, hops, after)
                blocks.update(zip(hops, packed))
                after = (packed[-1],)
            for j in HOPS:
                blocks[j] = lax.ppermute(blocks[j], "tp", [(i, (i + j) % n) for i in range(n)])
            blocks = [blocks[j] for j in range(n)]
            arrived.append(blocks)

        group = query.shape[1]
        out = pl.pallas_call(
            attend_kernel,
            out_shape=jax.ShapeDtypeStruct(query.shape, query.dtype),
            in_specs=[hbm] * 7,
            out_specs=pl.BlockSpec(memory_space=pltpu.VMEM),
            scratch_shapes=[
                pltpu.SMEM((batch,), jnp.int32),
                pltpu.VMEM(query.shape, query.dtype),
                pltpu.VMEM((2, batch, head_dim), dtype),
                pltpu.VMEM((2, batch, head_dim), jnp.float32),
                pltpu.VMEM((2, 2, seq_len, head_dim), dtype),
                pltpu.SemaphoreType.DMA((4,)),
                pltpu.SemaphoreType.DMA((2,)),
            ],
            compiler_params=pltpu.CompilerParams(vmem_limit_bytes=LESS_BYTES),
            cost_estimate=cost(4 * batch * group * seq_len * head_dim, batch * row_bytes),
            name="attend",
        )(lens, query, new_k, new_v, keys, values, *after)

        outs = ()
        for reqs, blocks in zip(pieces, arrived):
            outs = unpack(reqs, blocks, outs)
        return out, *outs

    head_spec = P("dp", "tp")
    entry_spec = P("dp", None, "tp")
    return jax.shard_map(layer, mesh=mesh, in_specs=(head_spec, entry_spec, entry_spec, head_spec, head_spec, P("dp")), out_specs=(head_spec, P("dp", "tp"), P("dp", "tp")), check_vma=False)
```
